32 devices in a mesh: groups: 2 (over y), ctx: 4 (over z), ep: 2 (over x), tp: 2 (over core).
Axes of the slice: x: 2, y: 2, z: 4, core: 2. Of those that a mesh axis runs over, the one named last changes fastest.
Arguments:
- queries: bfloat16 [4, 512, 5120], P(('groups', 'ep'), 'ctx', 'tp'), parts along dimension 0, may hold values from -128 to 128
- keys: bfloat16 [4, 512, 1024], P(('groups', 'ep'), 'ctx', 'tp'), parts along dimension 0, may hold values from -6 to 6
- values: bfloat16 [4, 512, 1024], P(('groups', 'ep'), 'ctx', 'tp'), parts along dimension 0, may hold values from -6 to 6
- expert_ids: int32 [4, 512, 1], P(('groups', 'ep'), 'ctx'), parts along dimension 0, may hold values from 0 to 127, as said below
- router: bfloat16 [5120, 2], P('tp', 'ep'), may hold values from -0.3125 to 0.3125
- w_gate: bfloat16 [2, 5120, 4096], P('ep', 'tp', 'ctx'), may hold values from -0.3125 to 0.3125
- w_up: bfloat16 [2, 5120, 4096], P('ep', 'tp', 'ctx'), may hold values from -0.3125 to 0.3125
- w_down: bfloat16 [2, 4096, 5120], P('ep', 'ctx', 'tp'), may hold values from -0.09375 to 0.09375
Outputs:
- layer_out: bfloat16 [4, 512, 5120], P(('groups', 'ep'), 'ctx', 'tp'), parts along dimension 0
The draws below stay inside these ranges and needn't reach their ends.
There are 2 independent parts, one for each index of `groups`. The reference program is written for one: setup_inputs(seed, part) draws one part's arguments, and reference() takes and returns one part's arrays. A program takes and returns all parts, laid end to end along the dimension named above; an argument that names none is the same for every part. Nothing has to cross between parts.
Inputs may be any that keep to these rules, and one draw needn't show every extreme that they name: `expert_ids`: among the positions of one device, each expert below 2 is named at most 2 times; in every draw one of them is named exactly 2 times on every device.
All inputs are finite; a program needn't handle non-finite values.
Results may differ from the reference program's by a relative error of at most 0.023.
Values may be sent and summed in bfloat16 or wider, within the bound.
A program may use at most 64 MiB of HBM per device.

```python
import math
import jax
import jax.numpy as jnp
from jax import lax

HEAD_WIDTH = 128
QUERY_HEADS = 40
KEY_VALUE_HEADS = 8
D = 5120
EXPERTS = 128
FE = 4096
SEQ_DEV = 128
PROMPT_LENGTH = 512
PROMPT_BATCH = 2
EXP_WIN = 2
CAP = 2


def shared_keys(key):
    return jax.random.truncated_normal(jax.random.fold_in(key, 11), -6.0, 6.0, (PROMPT_BATCH, PROMPT_LENGTH, KEY_VALUE_HEADS, HEAD_WIDTH), jnp.float32)


def draw_keys(key, part):
    unprojected_keys = shared_keys(key)
    return unprojected_keys.reshape(PROMPT_BATCH, PROMPT_LENGTH, KEY_VALUE_HEADS * HEAD_WIDTH).astype(jnp.bfloat16)


def draw_queries(key, part):
    base = 2.5 * jax.random.truncated_normal(jax.random.fold_in(key, 23), -6.0, 6.0, (PROMPT_BATCH, PROMPT_LENGTH, QUERY_HEADS, HEAD_WIDTH), jnp.float32)
    return base.reshape(PROMPT_BATCH, PROMPT_LENGTH, QUERY_HEADS * HEAD_WIDTH).astype(jnp.bfloat16)


def shuffled(sub_key):
    return jax.random.permutation(sub_key, SEQ_DEV)


def draw_expert_ids(key, part):
    blocks = PROMPT_BATCH * (PROMPT_LENGTH // SEQ_DEV)
    count_key = jax.random.fold_in(key, 41)
    full_key = jax.random.fold_in(key, 43)
    outside_key = jax.random.fold_in(key, 47)
    order_key = jax.random.fold_in(key, 53)
    counts = jax.random.randint(count_key, (blocks, EXP_WIN), 0, CAP + 1, dtype=jnp.int32)
    full_expert = jax.random.randint(full_key, (), 0, EXP_WIN, dtype=jnp.int32)
    counts = jnp.where(jnp.arange(EXP_WIN, dtype=jnp.int32)[None, :] == full_expert, CAP, counts)
    count_ends = jnp.cumsum(counts, axis=1)
    rank_index = jnp.arange(SEQ_DEV, dtype=jnp.int32)
    expert_rank = jnp.sum((count_ends[:, None, :] <= rank_index[None, :, None]).astype(jnp.int32), axis=2)
    outside = jax.random.randint(outside_key, (blocks, SEQ_DEV), EXP_WIN, EXPERTS, dtype=jnp.int32)
    named = jnp.where(expert_rank < EXP_WIN, expert_rank, outside)
    shuffles = jax.vmap(shuffled)(jax.random.split(order_key, blocks))
    inverse = jnp.argsort(shuffles, axis=1)
    placed = jnp.take_along_axis(named, inverse, axis=1)
    return placed.reshape(PROMPT_BATCH, PROMPT_LENGTH, 1).astype(jnp.int32)


def block_levels(stream_key, shape, cuts, smallest, largest):
    gain = 1.0
    for dim, parts in cuts:
        steps = jax.random.uniform(jax.random.fold_in(jax.random.fold_in(stream_key, 6), dim), (parts,), jnp.float32, smallest / len(cuts), largest / len(cuts))
        gain = gain * jnp.repeat(jnp.exp(steps), shape[dim] // parts).reshape((-1,) + (1,) * (len(shape) - 1 - dim))
    return gain


def normal_values(stream_key, dims, deviation, most, cuts=(), kind=jnp.bfloat16):
    drawn = deviation * jax.random.normal(stream_key, dims, jnp.float32)
    if cuts:
        drawn = drawn * block_levels(stream_key, dims, cuts, -0.22, 0.18)
    return jnp.clip(drawn, -most, most).astype(kind)


def setup_inputs(seed: int = 0, part: int = 0) -> dict:
    arg_keys = jax.random.split(jax.random.key(seed), 9)
    own_keys = jax.random.split(jax.random.fold_in(arg_keys[8], part), 9)
    return {
        "queries": draw_queries(jax.random.fold_in(jax.random.fold_in(arg_keys[8], part), 71), part),
        "keys": draw_keys(jax.random.fold_in(jax.random.fold_in(arg_keys[8], part), 71), part),
        "values": normal_values(own_keys[2], (PROMPT_BATCH, PROMPT_LENGTH, KEY_VALUE_HEADS * HEAD_WIDTH), 1.0, 6.0, ((0, 2), (1, 4), (2, 2))),
        "expert_ids": draw_expert_ids(jax.random.fold_in(jax.random.fold_in(arg_keys[8], part), 71), part),
        "router": normal_values(arg_keys[4], (D, EXP_WIN), (D // 16) ** -0.5, 0.3125, ((0, 2), (1, 2))),
        "w_gate": normal_values(arg_keys[5], (EXP_WIN, D, FE), (D // 16) ** -0.5, 0.3125, ((0, 2), (1, 2), (2, 4))),
        "w_up": normal_values(arg_keys[6], (EXP_WIN, D, FE), (D // 16) ** -0.5, 0.3125, ((0, 2), (1, 2), (2, 4))),
        "w_down": normal_values(arg_keys[7], (EXP_WIN, FE, D), FE ** -0.5, 0.09375, ((0, 2), (1, 4), (2, 2))),
    }


def attend_sequence(query_sequence, key_sequence, value_sequence):
    group_width = QUERY_HEADS // KEY_VALUE_HEADS
    rows_per_block = math.gcd(PROMPT_LENGTH, 256)
    query_block_list = query_sequence.reshape(PROMPT_LENGTH // rows_per_block, rows_per_block, KEY_VALUE_HEADS, group_width, HEAD_WIDTH)
    complete_keys = key_sequence.reshape(PROMPT_LENGTH, KEY_VALUE_HEADS, HEAD_WIDTH).astype(jnp.float32)
    complete_values = value_sequence.reshape(PROMPT_LENGTH, KEY_VALUE_HEADS, HEAD_WIDTH).astype(jnp.float32)
    key_pos = jnp.arange(PROMPT_LENGTH, dtype=jnp.int32)

    def one_block(inputs):
        query_block, begin_row = inputs
        scores = jnp.einsum("rgqd,kgd->gqrk", query_block.astype(jnp.float32), complete_keys) * (HEAD_WIDTH ** -0.5)
        query_pos = begin_row + jnp.arange(rows_per_block, dtype=jnp.int32)
        visible = query_pos[:, None] >= key_pos[None, :]
        scores = jnp.where(visible, scores, -1e30)
        row_max = jnp.max(scores, axis=3, keepdims=True)
        weights = jnp.where(visible, jnp.exp(scores - row_max), 0.0)
        totals = jnp.sum(weights, axis=3)
        rounded = lax.optimization_barrier(weights.astype(jnp.bfloat16)).astype(jnp.float32)
        weighted = jnp.einsum("gqrk,kgd->rgqd", rounded, complete_values)
        normed = weighted / jnp.transpose(totals, (2, 0, 1))[..., None]
        return normed.astype(jnp.bfloat16).reshape(rows_per_block, D)

    starts = jnp.arange(PROMPT_LENGTH // rows_per_block, dtype=jnp.int32) * rows_per_block
    return lax.map(one_block, (query_block_list, starts)).reshape(PROMPT_LENGTH, D)


def reference(queries, keys, values, expert_ids, router, w_gate, w_up, w_down):
    attended = jnp.stack([attend_sequence(queries[prompt], keys[prompt], values[prompt]) for prompt in range(PROMPT_BATCH)])
    token_count = PROMPT_BATCH * PROMPT_LENGTH
    flat_tokens = attended.reshape(token_count, D)
    chosen = expert_ids.reshape(token_count).astype(jnp.int32)
    sort_order = jnp.argsort(chosen, stable=True).astype(jnp.int32)
    counts = jnp.sum((chosen[:, None] == jnp.arange(EXP_WIN, dtype=jnp.int32)[None, :]).astype(jnp.int32), axis=0)
    offsets = (jnp.cumsum(counts) - counts).astype(jnp.int32)
    most_rows = CAP * PROMPT_BATCH * (PROMPT_LENGTH // SEQ_DEV)
    padded_order = jnp.concatenate([sort_order, jnp.zeros((most_rows,), jnp.int32)])

    def expert_step(routed, inputs):
        expert, gate_w, up_w, down_w, router_col = inputs
        picked = lax.dynamic_slice_in_dim(padded_order, offsets[expert], most_rows)
        live_rows = jnp.arange(most_rows, dtype=jnp.int32) < counts[expert]
        members = flat_tokens[picked]
        gate_part = jnp.dot(members, gate_w, preferred_element_type=jnp.float32)
        up_part = jnp.dot(members, up_w, preferred_element_type=jnp.float32)
        router_score = jnp.dot(members, router_col[:, None], preferred_element_type=jnp.float32)
        weight = jax.nn.sigmoid(router_score)
        hidden = (jax.nn.silu(weight * gate_part) * (weight * up_part)).astype(jnp.bfloat16)
        output = jnp.dot(hidden, down_w, preferred_element_type=jnp.float32).astype(jnp.bfloat16)
        output = lax.optimization_barrier(output).astype(jnp.float32)
        output = jnp.where(live_rows[:, None], output, 0.0)
        return routed.at[picked].add(output), None

    routed, _ = lax.scan(expert_step, jnp.zeros((token_count, D), jnp.float32),
                         (jnp.arange(EXP_WIN, dtype=jnp.int32), w_gate, w_up, w_down, router.T))
    layer_out = (flat_tokens.astype(jnp.float32) + routed).astype(jnp.bfloat16)
    return layer_out.reshape(PROMPT_BATCH, PROMPT_LENGTH, D)
```

```python
import functools
import math

import jax
import jax.numpy as jnp
from jax import lax
from jax.experimental import pallas as pl
from jax.experimental.pallas import tpu as pltpu
from jax.sharding import PartitionSpec as P

HEAD_WIDTH = 128
CAP = 2
MESH = pl.DeviceIdType.MESH
MASKED = -1e30
EXP2_SCALE = HEAD_WIDTH ** (-0.5) * math.log2(math.e)


def tiles_of(width, tile):
    tile = min(width, tile)
    return [(start, min(tile, width - start)) for start in range(0, width, tile)]


def each(count, body):
    if count <= 8:
        for index in range(count):
            body(index)
    else:
        pl.loop(0, count)(body)


def kernel(
    n_ctx, n_ep, n_tp,
    ids_ref, router_ref, q_ref, k_ref, v_ref, wg_hbm, wu_hbm, wd_hbm,
    out_ref,
    wg, wu, wd, kbuf, vbuf, acc, row_max, totals, att,
    out_rows, in_rows, members_f32, part, part_in, score, score_in, hidden,
    down_out, down_in, returned,
    w_sem, kv_send, kv_recv, row_send, row_recv, part_send, part_recv, score_sem,
    down_send, down_recv,
):
    ctx = lax.axis_index("ctx")
    ep = lax.axis_index("ep")
    tp = lax.axis_index("tp")
    n = n_ctx * n_ep
    me = ep * n_ctx + ctx
    rows = q_ref.shape[1]
    features = q_ref.shape[2]
    kv_heads = k_ref.shape[2] // HEAD_WIDTH
    group = features // HEAD_WIDTH // kv_heads
    half = rows // 2
    fan = n_ctx // 2
    hidden_width = wg.shape[1]
    chunk_count, _, double_width = part.shape
    chunk_width = double_width // 2
    slots = returned.shape[0]

    w_copies = [
        pltpu.make_async_copy(src.at[0], dst, w_sem.at[index])
        for index, (src, dst) in enumerate(((wg_hbm, wg), (wu_hbm, wu), (wd_hbm, wd)))
    ]
    for copy in w_copies:
        copy.start()

    barrier = pltpu.get_barrier_semaphore()

    def greet(other):
        @pl.when(other != me)
        def _():
            pl.semaphore_signal(
                barrier, inc=1,
                device_id={"ep": other // n_ctx, "ctx": other % n_ctx},
                device_id_type=MESH,
            )

    each(n, greet)
    for step in range(1, n_tp):
        pl.semaphore_signal(
            barrier, inc=1, device_id={"tp": (tp + step) % n_tp}, device_id_type=MESH
        )
    pl.semaphore_wait(barrier, n - 1 + n_tp - 1)

    right = (ctx + 1) % n_ctx
    left = (ctx + n_ctx - 1) % n_ctx

    def kv_copies(block, piece, direction, own):
        span = pl.ds(piece * half, half)
        target = right if direction == 0 else left
        result = []
        for index, (src, buf) in enumerate(((k_ref, kbuf), (v_ref, vbuf))):
            origin = src.at[0, span] if own else buf.at[block, span]
            result.append(
                pltpu.make_async_remote_copy(
                    src_ref=origin,
                    dst_ref=buf.at[block, span],
                    send_sem=kv_send.at[direction, block, piece, index],
                    recv_sem=kv_recv.at[block, piece, index],
                    device_id={"ctx": target},
                    device_id_type=MESH,
                )
            )
        return result

    def send_kv(block, piece, direction, own=False):
        for copy in kv_copies(block, piece, direction, own):
            copy.start()

    def wait_kv(block, piece):
        for copy in kv_copies(block, piece, 0, False):
            copy.wait_recv()

    send_kv(ctx, 0, 0, True)
    send_kv(ctx, 1, 1, True)
    if fan > 1:
        send_kv(ctx, 1, 0, True)
        send_kv(ctx, 0, 1, True)

    kbuf[ctx] = k_ref[0]
    vbuf[ctx] = v_ref[0]
    acc[...] = jnp.zeros_like(acc)
    totals[...] = jnp.zeros_like(totals)
    row_max[...] = jnp.full_like(row_max, MASKED)

    ids = ids_ref[...]
    slot_row = lax.broadcasted_iota(jnp.int32, (slots, rows), 0)
    choose = jnp.where(ids == slot_row, 1.0, 0.0)
    below = lax.broadcasted_iota(jnp.int32, (rows, rows), 0)
    across = lax.broadcasted_iota(jnp.int32, (rows, rows), 1)
    strict = jnp.where(below < across, 1.0, 0.0).astype(jnp.bfloat16)
    earlier = jnp.dot(choose.astype(jnp.bfloat16), strict, preferred_element_type=jnp.float32)
    slot_index = jnp.sum(earlier * choose, axis=0, keepdims=True).astype(jnp.int32)
    target_row = jnp.where(ids < n_ep, ids * CAP + slot_index, -1)
    spread = jnp.where(target_row == slot_row, 1.0, 0.0).astype(jnp.bfloat16)
    query_offset = lax.broadcasted_iota(jnp.int32, (rows, rows), 0)
    key_offset = lax.broadcasted_iota(jnp.int32, (rows, rows), 1)
    offset_gap = query_offset - key_offset

    def process(block):
        visible = offset_gap >= (block - ctx) * rows
        visible = jnp.concatenate([visible] * group, axis=0)
        for head in range(kv_heads):
            lanes = slice(head * HEAD_WIDTH, (head + 1) * HEAD_WIDTH)
            stacked = jnp.concatenate(
                [
                    q_ref[0, :, (head * group + j) * HEAD_WIDTH:(head * group + j + 1) * HEAD_WIDTH]
                    for j in range(group)
                ],
                axis=0,
            )
            raw = lax.dot_general(
                stacked, kbuf[block, :, lanes], (((1,), (1,)), ((), ())),
                preferred_element_type=jnp.float32,
            )
            raw = jnp.where(visible, raw, MASKED)
            old_max = row_max[head]
            new_max = jnp.maximum(old_max, jnp.max(raw, axis=1, keepdims=True))
            factor = jnp.exp2((old_max - new_max) * EXP2_SCALE)
            weights = jnp.exp2((raw - new_max[:, :rows]) * EXP2_SCALE)
            row_max[head] = new_max
            totals[head] = totals[head] * factor + jnp.sum(weights, axis=1, keepdims=True)
            update = jnp.dot(
                weights.astype(jnp.bfloat16), vbuf[block, :, lanes],
                preferred_element_type=jnp.float32,
            )
            acc[head] = acc[head] * factor + update

    def visit(index, carry):
        step = (index + 1) // 2

        @pl.when((index % 2 == 1) & (index < n_ctx - 1))
        def _():
            from_left = (ctx + n_ctx - step) % n_ctx
            from_right = (ctx + step) % n_ctx
            wait_kv(from_left, 0)
            send_kv(from_left, 0, 0)
            wait_kv(from_right, 1)
            send_kv(from_right, 1, 1)
            wait_kv(from_left, 1)

            @pl.when(step + 1 < fan)
            def _():
                send_kv(from_left, 1, 0)

            wait_kv(from_right, 0)

            @pl.when(step + 1 < fan)
            def _():
                send_kv(from_right, 0, 1)

        block = jnp.where(index % 2 == 1, ctx + n_ctx - step, ctx + step) % n_ctx

        @pl.when(index == n_ctx - 1)
        def _():
            wait_kv(block, 0)
            wait_kv(block, 1)

        @pl.when(block <= ctx)
        def _():
            process(block)

        return carry

    lax.fori_loop(0, n_ctx, visit, 0)

    for head in range(kv_heads):
        normed = (acc[head] / totals[head]).astype(jnp.bfloat16)
        for j in range(group):
            place = (head * group + j) * HEAD_WIDTH
            att[:, place:place + HEAD_WIDTH] = normed[j * rows:(j + 1) * rows]

    for start, size in tiles_of(features, 512):
        picked = jnp.dot(
            spread, att[:, start:start + size], preferred_element_type=jnp.float32
        )
        for expert in range(n_ep):
            out_rows[expert, :, start:start + size] = picked[
                expert * CAP:(expert + 1) * CAP
            ].astype(jnp.bfloat16)

    def row_copy(other, source):
        return pltpu.make_async_remote_copy(
            src_ref=out_rows.at[other // n_ctx],
            dst_ref=in_rows.at[source],
            send_sem=row_send.at[other],
            recv_sem=row_recv.at[source],
            device_id={"ep": other // n_ctx, "ctx": other % n_ctx},
            device_id_type=MESH,
        )

    def others(body):
        def one(step):
            @pl.when(step != me)
            def _():
                body(step)

        each(n, one)

    others(lambda other: row_copy(other, me).start())
    in_rows[me] = out_rows[ep]
    for copy in w_copies:
        copy.wait()
    others(lambda other: row_copy(other, other).wait_recv())

    def gather_member(index):
        members_f32[index * CAP:(index + 1) * CAP, :] = in_rows[index].astype(jnp.float32)

    for index in range(n):
        gather_member(index)
    wide = members_f32[...]
    members = wide.astype(jnp.bfloat16)
    own_score = jnp.sum(wide * router_ref[...].astype(jnp.float32), axis=1, keepdims=True)
    score[...] = jnp.broadcast_to(own_score, score.shape).astype(jnp.bfloat16)
    peer = {"tp": n_tp - 1 - tp}
    score_copy = pltpu.make_async_remote_copy(
        src_ref=score, dst_ref=score_in, send_sem=score_sem.at[0], recv_sem=score_sem.at[1],
        device_id=peer, device_id_type=MESH,
    )
    score_copy.start()
    part_copies = []
    for chunk in range(chunk_count):
        span = slice(chunk * chunk_width, (chunk + 1) * chunk_width)
        part[chunk, :, :chunk_width] = jnp.dot(
            members, wg[:, span], preferred_element_type=jnp.float32
        ).astype(jnp.bfloat16)
        part[chunk, :, chunk_width:] = jnp.dot(
            members, wu[:, span], preferred_element_type=jnp.float32
        ).astype(jnp.bfloat16)
        copy = pltpu.make_async_remote_copy(
            src_ref=part.at[chunk], dst_ref=part_in.at[chunk],
            send_sem=part_send.at[chunk], recv_sem=part_recv.at[chunk],
            device_id=peer, device_id_type=MESH,
        )
        copy.start()
        part_copies.append(copy)
    score_copy.wait()
    gain = jax.nn.sigmoid(
        score[:, :1].astype(jnp.float32) + score_in[:, :1].astype(jnp.float32)
    )
    for chunk, copy in enumerate(part_copies):
        copy.wait()
        both = part[chunk].astype(jnp.float32) + part_in[chunk].astype(jnp.float32)
        gate = gain * both[:, :chunk_width]
        up = gain * both[:, chunk_width:]
        hidden[:, chunk * chunk_width:(chunk + 1) * chunk_width] = (
            gate * jax.nn.sigmoid(gate) * up
        ).astype(jnp.bfloat16)
    for start, size in tiles_of(features, 512):
        product = jnp.dot(
            hidden[...], wd[:, start:start + size], preferred_element_type=jnp.float32
        )
        for index in range(n):
            down_out[index, :, start:start + size] = product[
                index * CAP:(index + 1) * CAP
            ].astype(jnp.bfloat16)

    def down_copy(other, source):
        return pltpu.make_async_remote_copy(
            src_ref=down_out.at[other],
            dst_ref=down_in.at[source],
            send_sem=down_send.at[other],
            recv_sem=down_recv.at[source],
            device_id={"ep": other // n_ctx, "ctx": other % n_ctx},
            device_id_type=MESH,
        )

    others(lambda other: down_copy(other, me).start())
    down_in[me] = down_out[me]
    returned[...] = jnp.zeros_like(returned)

    others(lambda other: row_copy(other, me).wait_send())
    for copy in kv_copies(ctx, 0, 0, True) + kv_copies(ctx, 1, 1, True):
        copy.wait_send()
    if fan > 1:
        for copy in kv_copies(ctx, 1, 0, True) + kv_copies(ctx, 0, 1, True):
            copy.wait_send()

    def drain(step, carry):
        from_left = (ctx + n_ctx - step) % n_ctx
        from_right = (ctx + step) % n_ctx
        for copy in kv_copies(from_left, 0, 0, False) + kv_copies(from_right, 1, 1, False):
            copy.wait_send()

        @pl.when(step + 1 < fan)
        def _():
            for copy in kv_copies(from_left, 1, 0, False) + kv_copies(from_right, 0, 1, False):
                copy.wait_send()

        return carry

    lax.fori_loop(1, fan, drain, 0)

    others(lambda other: down_copy(other, other).wait_recv())
    for expert in range(n_ep):
        total = down_in[expert * n_ctx].astype(jnp.float32)
        for index in range(1, n_ctx):
            total = total + down_in[expert * n_ctx + index].astype(jnp.float32)
        returned[expert * CAP:(expert + 1) * CAP, :] = total.astype(jnp.bfloat16).astype(jnp.float32)
    for start, size in tiles_of(features, 512):
        routed = lax.dot_general(
            spread, returned[:, start:start + size].astype(jnp.bfloat16),
            (((0,), (0,)), ((), ())), preferred_element_type=jnp.float32,
        )
        out_ref[0, :, start:start + size] = (
            att[:, start:start + size].astype(jnp.float32) + routed
        ).astype(jnp.bfloat16)
    others(lambda other: down_copy(other, me).wait_send())


def shards(queries, keys, values, expert_ids, router, w_gate, w_up, w_down):
    n_ctx, n_ep, n_tp = (lax.axis_size(axis) for axis in ("ctx", "ep", "tp"))
    n = n_ctx * n_ep
    _, rows, features = queries.shape
    kv_width = keys.shape[2]
    kv_heads = kv_width // HEAD_WIDTH
    group = features // kv_width
    hidden_width = w_gate.shape[2]
    chunk_width = min(hidden_width, 256)
    chunk_count = hidden_width // chunk_width
    members = n * CAP
    slots = -(-n_ep * CAP // 8) * 8
    bf16, f32 = jnp.bfloat16, jnp.float32
    vmem = pl.BlockSpec(memory_space=pltpu.VMEM)
    hbm = pl.BlockSpec(memory_space=pl.ANY)
    dma = pltpu.SemaphoreType.DMA
    return pl.pallas_call(
        functools.partial(kernel, n_ctx, n_ep, n_tp),
        out_shape=jax.ShapeDtypeStruct(queries.shape, bf16),
        in_specs=[vmem] * 5 + [hbm] * 3,
        out_specs=vmem,
        scratch_shapes=[
            pltpu.VMEM(w_gate.shape[1:], bf16),
            pltpu.VMEM(w_up.shape[1:], bf16),
            pltpu.VMEM(w_down.shape[1:], bf16),
            pltpu.VMEM((n_ctx, rows, kv_width), bf16),
            pltpu.VMEM((n_ctx, rows, kv_width), bf16),
            pltpu.VMEM((kv_heads, group * rows, HEAD_WIDTH), f32),
            pltpu.VMEM((kv_heads, group * rows, HEAD_WIDTH), f32),
            pltpu.VMEM((kv_heads, group * rows, HEAD_WIDTH), f32),
            pltpu.VMEM((rows, features), bf16),
            pltpu.VMEM((n_ep, CAP, features), bf16),
            pltpu.VMEM((n, CAP, features), bf16),
            pltpu.VMEM((members, features), f32),
            pltpu.VMEM((chunk_count, members, 2 * chunk_width), bf16),
            pltpu.VMEM((chunk_count, members, 2 * chunk_width), bf16),
            pltpu.VMEM((members, 128), bf16),
            pltpu.VMEM((members, 128), bf16),
            pltpu.VMEM((members, hidden_width), bf16),
            pltpu.VMEM((n, CAP, features), bf16),
            pltpu.VMEM((n, CAP, features), bf16),
            pltpu.VMEM((slots, features), f32),
            dma((3,)),
            dma((2, n_ctx, 2, 2)),
            dma((n_ctx, 2, 2)),
            dma((n,)),
            dma((n,)),
            dma((chunk_count,)),
            dma((chunk_count,)),
            dma((2,)),
            dma((n,)),
            dma((n,)),
        ],
        compiler_params=pltpu.CompilerParams(
            collective_id=0, has_side_effects=True, vmem_limit_bytes=60 * 1024 * 1024
        ),
    )(
        expert_ids.reshape(1, rows), router.reshape(1, features), queries, keys, values,
        w_gate, w_up, w_down,
    )


def solution(mesh):
    placed = (
        P(("groups", "ep"), "ctx", "tp"),
        P(("groups", "ep"), "ctx", "tp"),
        P(("groups", "ep"), "ctx", "tp"),
        P(("groups", "ep"), "ctx", None),
        P("tp", "ep"),
        P("ep", "tp", "ctx"),
        P("ep", "tp", "ctx"),
        P("ep", "ctx", "tp"),
    )
    return jax.shard_map(
        shards,
        mesh=mesh,
        in_specs=placed,
        out_specs=P(("groups", "ep"), "ctx", "tp"),
        check_vma=False,
    )
```

```python
import functools
import math

import jax
import jax.numpy as jnp
from jax import lax
from jax.experimental import pallas as pl
from jax.experimental.pallas import tpu as pltpu
from jax.sharding import PartitionSpec as P

HEAD_WIDTH = 128
CAP = 2
MESH = pl.DeviceIdType.MESH
MASKED = -1e30
EXP2_SCALE = HEAD_WIDTH ** (-0.5) * math.log2(math.e)


def tiles_of(width, tile):
    tile = min(width, tile)
    return [(start, min(tile, width - start)) for start in range(0, width, tile)]


def each(count, body):
    if count <= 8:
        for index in range(count):
            body(index)
    else:
        pl.loop(0, count)(body)


def kernel(
    n_ctx, n_ep, n_tp,
    ids_ref, router_ref, q_ref, k_ref, v_ref, wg_hbm, wu_hbm, wd_hbm,
    out_ref,
    wg, wu, wd, kbuf, vbuf, acc, row_max, totals, att,
    q_out, q_in, q_all, part_out, part_got, part_all, lse_out, lse_in, lse_all, out_rows, in_rows, members_f32, part, part_in, score, score_in, hidden,
    down_out, down_in, returned,
    w_sem, kv_send, kv_recv, row_send, row_recv, part_send, part_recv, score_sem,
    down_send, down_recv, q_send, q_recv, back_send, back_recv, lse_send, lse_recv,
):
    ctx = lax.axis_index("ctx")
    ep = lax.axis_index("ep")
    tp = lax.axis_index("tp")
    n = n_ctx * n_ep
    me = ep * n_ctx + ctx
    rows = q_ref.shape[1]
    features = q_ref.shape[2]
    kv_heads = k_ref.shape[2] // HEAD_WIDTH
    group = features // HEAD_WIDTH // kv_heads
    half = rows // 2
    fan = n_ctx // 2
    hidden_width = wg.shape[1]
    chunk_count, _, double_width = part.shape
    chunk_width = double_width // 2
    slots = returned.shape[0]

    w_copies = [
        pltpu.make_async_copy(src.at[0], dst, w_sem.at[index])
        for index, (src, dst) in enumerate(((wg_hbm, wg), (wu_hbm, wu), (wd_hbm, wd)))
    ]
    for copy in w_copies:
        copy.start()

    ids = ids_ref[...]
    slot_row = lax.broadcasted_iota(jnp.int32, (slots, rows), 0)
    choose = jnp.where(ids == slot_row, 1.0, 0.0)
    below = lax.broadcasted_iota(jnp.int32, (rows, rows), 0)
    across = lax.broadcasted_iota(jnp.int32, (rows, rows), 1)
    strict = jnp.where(below < across, 1.0, 0.0).astype(jnp.bfloat16)
    earlier = jnp.dot(choose.astype(jnp.bfloat16), strict, preferred_element_type=jnp.float32)
    slot_index = jnp.sum(earlier * choose, axis=0, keepdims=True).astype(jnp.int32)
    target_row = jnp.where(ids < n_ep, ids * CAP + slot_index, -1)
    spread = jnp.where(target_row == slot_row, 1.0, 0.0).astype(jnp.bfloat16)
    live = n_ep * CAP
    lane_row = lax.broadcasted_iota(jnp.int32, (slots, rows), 1)
    row_place = jnp.sum(
        jnp.where(target_row == slot_row, lane_row, 0), axis=1, keepdims=True
    )
    q_all[...] = jnp.zeros_like(q_all)
    own_span = pl.ds(pl.multiple_of(ctx * slots, 8), slots)
    for start, size in tiles_of(features, 512):
        picked = jnp.dot(
            spread, q_ref[0, :, start:start + size], preferred_element_type=jnp.float32
        )
        q_all[own_span, start:start + size] = picked
        q_out[:, start:start + size] = picked[:live].astype(jnp.bfloat16)

    barrier = pltpu.get_barrier_semaphore()

    def greet(other):
        @pl.when(other != me)
        def _():
            pl.semaphore_signal(
                barrier, inc=1,
                device_id={"ep": other // n_ctx, "ctx": other % n_ctx},
                device_id_type=MESH,
            )

    each(n, greet)
    for step in range(1, n_tp):
        pl.semaphore_signal(
            barrier, inc=1, device_id={"tp": (tp + step) % n_tp}, device_id_type=MESH
        )
    pl.semaphore_wait(barrier, n - 1 + n_tp - 1)

    def own_copy(piece):
        origin, buf = (k_ref, kbuf) if piece < 2 else (v_ref, vbuf)
        span = pl.ds((piece % 2) * half, half)
        return pltpu.make_async_remote_copy(
            src_ref=origin.at[0, span],
            dst_ref=buf.at[ctx, span],
            send_sem=kv_send.at[ctx, piece],
            recv_sem=kv_recv.at[ctx, piece],
            device_id={"ctx": ctx + 1},
            device_id_type=MESH,
        )

    def block_piece(block, piece):
        buf = kbuf if piece < 2 else vbuf
        span = pl.ds((piece % 2) * half, half)
        return pltpu.make_async_remote_copy(
            src_ref=buf.at[block, span],
            dst_ref=buf.at[block, span],
            send_sem=kv_send.at[block, piece],
            recv_sem=kv_recv.at[block, piece],
            device_id={"ctx": ctx + 1},
            device_id_type=MESH,
        )

    def push_own(first, last):
        @pl.when(ctx < n_ctx - 1)
        def _():
            for piece in range(first, last):
                own_copy(piece).start()

    def relay(block, first, last):
        @pl.when(block >= 0)
        def _():
            for piece in range(first, last):
                copy = block_piece(block, piece)
                copy.wait_recv()

                @pl.when(ctx < n_ctx - 1)
                def _():
                    copy.start()

    def q_copy(source, target):
        return pltpu.make_async_remote_copy(
            src_ref=q_out, dst_ref=q_in.at[source],
            send_sem=q_send.at[target], recv_sem=q_recv.at[source],
            device_id={"ctx": target}, device_id_type=MESH,
        )

    def back_copies(source, target):
        return [
            pltpu.make_async_remote_copy(
                src_ref=out.at[target], dst_ref=into.at[source],
                send_sem=sent.at[target], recv_sem=got.at[source],
                device_id={"ctx": target}, device_id_type=MESH,
            )
            for out, into, sent, got in (
                (part_out, part_got, back_send, back_recv),
                (lse_out, lse_in, lse_send, lse_recv),
            )
        ]

    def lower(body):
        def one(other):
            @pl.when(other < ctx)
            def _():
                body(other)

        each(n_ctx, one)

    def upper(body):
        def one(other):
            @pl.when(other > ctx)
            def _():
                body(other)

        each(n_ctx, one)

    lower(lambda other: q_copy(ctx, other).start())
    push_own(0, 2)

    kbuf[ctx] = k_ref[0]
    vbuf[ctx] = v_ref[0]
    acc[...] = jnp.zeros_like(acc)
    totals[...] = jnp.zeros_like(totals)
    row_max[...] = jnp.full_like(row_max, MASKED)

    query_offset = lax.broadcasted_iota(jnp.int32, (rows, rows), 0)
    key_offset = lax.broadcasted_iota(jnp.int32, (rows, rows), 1)
    offset_gap = query_offset - key_offset

    def process(block):
        visible = offset_gap >= (block - ctx) * rows
        visible = jnp.concatenate([visible] * group, axis=0)
        for head in range(kv_heads):
            lanes = slice(head * HEAD_WIDTH, (head + 1) * HEAD_WIDTH)
            stacked = jnp.concatenate(
                [
                    q_ref[0, :, (head * group + j) * HEAD_WIDTH:(head * group + j + 1) * HEAD_WIDTH]
                    for j in range(group)
                ],
                axis=0,
            )
            raw = lax.dot_general(
                stacked, kbuf[block, :, lanes], (((1,), (1,)), ((), ())),
                preferred_element_type=jnp.float32,
            )
            raw = jnp.where(visible, raw, MASKED)
            old_max = row_max[head]
            new_max = jnp.maximum(old_max, jnp.max(raw, axis=1, keepdims=True))
            factor = jnp.exp2((old_max - new_max) * EXP2_SCALE)
            weights = jnp.exp2((raw - new_max[:, :rows]) * EXP2_SCALE)
            row_max[head] = new_max
            totals[head] = totals[head] * factor + jnp.sum(weights, axis=1, keepdims=True)
            update = jnp.dot(
                weights.astype(jnp.bfloat16), vbuf[block, :, lanes],
                preferred_element_type=jnp.float32,
            )
            acc[head] = acc[head] * factor + update

    part_all[...] = jnp.zeros_like(part_all)
    lse_all[...] = jnp.full_like(lse_all, MASKED)
    source_row = lax.broadcasted_iota(jnp.int32, (n_ctx * slots, 1), 0) // slots
    limit = jnp.where(
        source_row == ctx, jnp.concatenate([row_place] * n_ctx, axis=0), rows
    )
    limit = jnp.concatenate([limit] * group, axis=0)
    upper(lambda other: q_copy(other, other).wait_recv())

    for other in range(n_ctx):
        @pl.when(other > ctx)
        def _():
            q_all[other * slots:other * slots + live, :] = q_in[other].astype(jnp.float32)

    tall = n_ctx * slots
    key_lane = lax.broadcasted_iota(jnp.int32, (group * tall, rows), 1)
    seen = key_lane <= limit
    head_lane = lax.broadcasted_iota(jnp.int32, (tall, 128), 1)
    lse = jnp.zeros((tall, 128), jnp.float32)
    for head in range(kv_heads):
        lanes = slice(head * HEAD_WIDTH, (head + 1) * HEAD_WIDTH)
        stacked = jnp.concatenate(
            [
                q_all[:, (head * group + j) * HEAD_WIDTH:(head * group + j + 1) * HEAD_WIDTH]
                for j in range(group)
            ],
            axis=0,
        ).astype(jnp.bfloat16)
        raw = lax.dot_general(
            stacked, k_ref[0, :, lanes], (((1,), (1,)), ((), ())),
            preferred_element_type=jnp.float32,
        )
        raw = jnp.where(seen, raw, MASKED)
        top = jnp.max(raw, axis=1, keepdims=True)
        weights = jnp.exp2((raw - top) * EXP2_SCALE)
        total = jnp.sum(weights, axis=1, keepdims=True)
        mixed = jnp.dot(
            weights.astype(jnp.bfloat16), v_ref[0, :, lanes],
            preferred_element_type=jnp.float32,
        ) / total
        column = top * EXP2_SCALE + jnp.log2(total)
        for j in range(group):
            place = head * group + j
            lse = jnp.where(head_lane == place, column[j * tall:(j + 1) * tall], lse)
            for other in range(n_ctx):
                first = j * tall + other * slots
                part_out[other, :, place * HEAD_WIDTH:(place + 1) * HEAD_WIDTH] = mixed[
                    first:first + live
                ].astype(jnp.bfloat16)
    for other in range(n_ctx):
        lse_out[other] = lse[other * slots:(other + 1) * slots]

    def give_back(other):
        for copy in back_copies(ctx, other):
            copy.start()

    upper(give_back)
    push_own(2, 4)

    def take_back(other):
        for copy in back_copies(other, other):
            copy.wait_recv()

    lower(take_back)
    for other in range(n_ctx):
        @pl.when(other < ctx)
        def _():
            part_all[other, :live] = part_got[other].astype(jnp.float32)
            lse_all[other] = lse_in[other]

        @pl.when(other == ctx)
        def _():
            part_all[other, :live] = part_out[other].astype(jnp.float32)
            lse_all[other] = lse_out[other]

    peak = jnp.max(lse_all[...], axis=0)
    shares = [jnp.exp2(lse_all[other] - peak) for other in range(n_ctx)]
    share_total = functools.reduce(jnp.add, shares)
    shares = [share / share_total for share in shares]
    for place in range(kv_heads * group):
        span = slice(place * HEAD_WIDTH, (place + 1) * HEAD_WIDTH)
        picked = shares[0][:, place:place + 1] * part_all[0, :, span]
        for other in range(1, n_ctx):
            picked = picked + shares[other][:, place:place + 1] * part_all[other, :, span]
        for expert in range(n_ep):
            out_rows[expert, :, span] = picked[expert * CAP:(expert + 1) * CAP].astype(
                jnp.bfloat16
            )

    def row_copy(other, source):
        return pltpu.make_async_remote_copy(
            src_ref=out_rows.at[other // n_ctx],
            dst_ref=in_rows.at[source],
            send_sem=row_send.at[other],
            recv_sem=row_recv.at[source],
            device_id={"ep": other // n_ctx, "ctx": other % n_ctx},
            device_id_type=MESH,
        )

    def others(body):
        def one(step):
            @pl.when(step != me)
            def _():
                body(step)

        each(n, one)

    others(lambda other: row_copy(other, me).start())
    in_rows[me] = out_rows[ep]
    process(ctx)
    relay(ctx - 1, 0, 2)
    for copy in w_copies:
        copy.wait()
    others(lambda other: row_copy(other, other).wait_recv())

    def gather_member(index):
        members_f32[index * CAP:(index + 1) * CAP, :] = in_rows[index].astype(jnp.float32)

    for index in range(n):
        gather_member(index)
    wide = members_f32[...]
    members = wide.astype(jnp.bfloat16)
    own_score = jnp.sum(wide * router_ref[...].astype(jnp.float32), axis=1, keepdims=True)
    score[...] = jnp.broadcast_to(own_score, score.shape).astype(jnp.bfloat16)
    peer = {"tp": n_tp - 1 - tp}
    score_copy = pltpu.make_async_remote_copy(
        src_ref=score, dst_ref=score_in, send_sem=score_sem.at[0], recv_sem=score_sem.at[1],
        device_id=peer, device_id_type=MESH,
    )
    score_copy.start()
    part_copies = []
    for chunk in range(chunk_count):
        span = slice(chunk * chunk_width, (chunk + 1) * chunk_width)
        part[chunk, :, :chunk_width] = jnp.dot(
            members, wg[:, span], preferred_element_type=jnp.float32
        ).astype(jnp.bfloat16)
        part[chunk, :, chunk_width:] = jnp.dot(
            members, wu[:, span], preferred_element_type=jnp.float32
        ).astype(jnp.bfloat16)
        copy = pltpu.make_async_remote_copy(
            src_ref=part.at[chunk], dst_ref=part_in.at[chunk],
            send_sem=part_send.at[chunk], recv_sem=part_recv.at[chunk],
            device_id=peer, device_id_type=MESH,
        )
        copy.start()
        part_copies.append(copy)
    relay(ctx - 1, 2, 4)
    score_copy.wait()
    gain = jax.nn.sigmoid(
        score[:, :1].astype(jnp.float32) + score_in[:, :1].astype(jnp.float32)
    )
    for chunk, copy in enumerate(part_copies):
        copy.wait()
        both = part[chunk].astype(jnp.float32) + part_in[chunk].astype(jnp.float32)
        gate = gain * both[:, :chunk_width]
        up = gain * both[:, chunk_width:]
        hidden[:, chunk * chunk_width:(chunk + 1) * chunk_width] = (
            gate * jax.nn.sigmoid(gate) * up
        ).astype(jnp.bfloat16)
    for start, size in tiles_of(features, 512):
        product = jnp.dot(
            hidden[...], wd[:, start:start + size], preferred_element_type=jnp.float32
        )
        for index in range(n):
            down_out[index, :, start:start + size] = product[
                index * CAP:(index + 1) * CAP
            ].astype(jnp.bfloat16)

    def down_copy(other, source):
        return pltpu.make_async_remote_copy(
            src_ref=down_out.at[other],
            dst_ref=down_in.at[source],
            send_sem=down_send.at[other],
            recv_sem=down_recv.at[source],
            device_id={"ep": other // n_ctx, "ctx": other % n_ctx},
            device_id_type=MESH,
        )

    others(lambda other: down_copy(other, me).start())
    down_in[me] = down_out[me]
    returned[...] = jnp.zeros_like(returned)

    def visit(step, carry):
        block = ctx - step

        @pl.when(step > 1)
        def _():
            relay(block, 0, 4)

        @pl.when(block >= 0)
        def _():
            process(block)

        return carry

    lax.fori_loop(1, n_ctx, visit, 0)

    for head in range(kv_heads):
        normed = (acc[head] / totals[head]).astype(jnp.bfloat16)
        for j in range(group):
            place = (head * group + j) * HEAD_WIDTH
            att[:, place:place + HEAD_WIDTH] = normed[j * rows:(j + 1) * rows]

    others(lambda other: row_copy(other, me).wait_send())
    lower(lambda other: q_copy(ctx, other).wait_send())

    def sent_back(other):
        for copy in back_copies(ctx, other):
            copy.wait_send()

    upper(sent_back)

    def drain(step, carry):
        block = ctx - step

        @pl.when((ctx < n_ctx - 1) & (block >= 0))
        def _():
            for piece in range(4):
                block_piece(block, piece).wait_send()

        return carry

    lax.fori_loop(0, n_ctx, drain, 0)

    others(lambda other: down_copy(other, other).wait_recv())
    for expert in range(n_ep):
        total = down_in[expert * n_ctx].astype(jnp.float32)
        for index in range(1, n_ctx):
            total = total + down_in[expert * n_ctx + index].astype(jnp.float32)
        returned[expert * CAP:(expert + 1) * CAP, :] = total.astype(jnp.bfloat16).astype(jnp.float32)
    for start, size in tiles_of(features, 512):
        routed = lax.dot_general(
            spread, returned[:, start:start + size].astype(jnp.bfloat16),
            (((0,), (0,)), ((), ())), preferred_element_type=jnp.float32,
        )
        out_ref[0, :, start:start + size] = (
            att[:, start:start + size].astype(jnp.float32) + routed
        ).astype(jnp.bfloat16)
    others(lambda other: down_copy(other, me).wait_send())


def shards(queries, keys, values, expert_ids, router, w_gate, w_up, w_down):
    n_ctx, n_ep, n_tp = (lax.axis_size(axis) for axis in ("ctx", "ep", "tp"))
    n = n_ctx * n_ep
    _, rows, features = queries.shape
    kv_width = keys.shape[2]
    kv_heads = kv_width // HEAD_WIDTH
    group = features // kv_width
    hidden_width = w_gate.shape[2]
    chunk_width = min(hidden_width, 256)
    chunk_count = hidden_width // chunk_width
    members = n * CAP
    live = n_ep * CAP
    slots = -(-live // 8) * 8
    bf16, f32 = jnp.bfloat16, jnp.float32
    vmem = pl.BlockSpec(memory_space=pltpu.VMEM)
    hbm = pl.BlockSpec(memory_space=pl.ANY)
    dma = pltpu.SemaphoreType.DMA
    return pl.pallas_call(
        functools.partial(kernel, n_ctx, n_ep, n_tp),
        out_shape=jax.ShapeDtypeStruct(queries.shape, bf16),
        in_specs=[vmem] * 5 + [hbm] * 3,
        out_specs=vmem,
        scratch_shapes=[
            pltpu.VMEM(w_gate.shape[1:], bf16),
            pltpu.VMEM(w_up.shape[1:], bf16),
            pltpu.VMEM(w_down.shape[1:], bf16),
            pltpu.VMEM((n_ctx, rows, kv_width), bf16),
            pltpu.VMEM((n_ctx, rows, kv_width), bf16),
            pltpu.VMEM((kv_heads, group * rows, HEAD_WIDTH), f32),
            pltpu.VMEM((kv_heads, group * rows, HEAD_WIDTH), f32),
            pltpu.VMEM((kv_heads, group * rows, HEAD_WIDTH), f32),
            pltpu.VMEM((rows, features), bf16),
            pltpu.VMEM((live, features), bf16),
            pltpu.VMEM((n_ctx, live, features), bf16),
            pltpu.VMEM((n_ctx * slots, features), f32),
            pltpu.VMEM((n_ctx, live, features), bf16),
            pltpu.VMEM((n_ctx, live, features), bf16),
            pltpu.VMEM((n_ctx, slots, features), f32),
            pltpu.VMEM((n_ctx, slots, 128), f32),
            pltpu.VMEM((n_ctx, slots, 128), f32),
            pltpu.VMEM((n_ctx, slots, 128), f32),
            pltpu.VMEM((n_ep, CAP, features), bf16),
            pltpu.VMEM((n, CAP, features), bf16),
            pltpu.VMEM((members, features), f32),
            pltpu.VMEM((chunk_count, members, 2 * chunk_width), bf16),
            pltpu.VMEM((chunk_count, members, 2 * chunk_width), bf16),
            pltpu.VMEM((members, 128), bf16),
            pltpu.VMEM((members, 128), bf16),
            pltpu.VMEM((members, hidden_width), bf16),
            pltpu.VMEM((n, CAP, features), bf16),
            pltpu.VMEM((n, CAP, features), bf16),
            pltpu.VMEM((slots, features), f32),
            dma((3,)),
            dma((n_ctx, 4)),
            dma((n_ctx, 4)),
            dma((n,)),
            dma((n,)),
            dma((chunk_count,)),
            dma((chunk_count,)),
            dma((2,)),
            dma((n,)),
            dma((n,)),
            dma((n_ctx,)),
            dma((n_ctx,)),
            dma((n_ctx,)),
            dma((n_ctx,)),
            dma((n_ctx,)),
            dma((n_ctx,)),
        ],
        compiler_params=pltpu.CompilerParams(
            collective_id=0, has_side_effects=True, vmem_limit_bytes=60 * 1024 * 1024
        ),
    )(
        expert_ids.reshape(1, rows), router.reshape(1, features), queries, keys, values,
        w_gate, w_up, w_down,
    )


def solution(mesh):
    placed = (
        P(("groups", "ep"), "ctx", "tp"),
        P(("groups", "ep"), "ctx", "tp"),
        P(("groups", "ep"), "ctx", "tp"),
        P(("groups", "ep"), "ctx", None),
        P("tp", "ep"),
        P("ep", "tp", "ctx"),
        P("ep", "tp", "ctx"),
        P("ep", "ctx", "tp"),
    )
    return jax.shard_map(
        shards,
        mesh=mesh,
        in_specs=placed,
        out_specs=P(("groups", "ep"), "ctx", "tp"),
        check_vma=False,
    )
```

```python
import functools
import math

import jax
import jax.numpy as jnp
from jax import lax
from jax.experimental import pallas as pl
from jax.experimental.pallas import tpu as pltpu
from jax.sharding import PartitionSpec as P

HEAD_WIDTH = 128
CAP = 2
MESH = pl.DeviceIdType.MESH
MASKED = -1e30
EXP2_SCALE = HEAD_WIDTH ** (-0.5) * math.log2(math.e)


def tiles_of(width, tile):
    tile = min(width, tile)
    return [(start, min(tile, width - start)) for start in range(0, width, tile)]


def each(count, body):
    if count <= 8:
        for index in range(count):
            body(index)
    else:
        pl.loop(0, count)(body)


def kernel(
    n_ctx, n_ep, n_tp,
    ids_ref, router_ref, q_ref, k_ref, v_ref, wg_hbm, wu_hbm, wd_hbm,
    out_ref,
    wg, wu, wd, kbuf, vbuf, acc, row_max, totals, att,
    q_out, q_in, q_all, part_out, part_got, part_all, lse_out, lse_in, lse_all, out_rows, in_rows, members_f32, part, part_in, score, score_in, hidden,
    down_out, down_in, returned,
    w_sem, kv_send, kv_recv, row_send, row_recv, part_send, part_recv, score_sem,
    down_send, down_recv, q_send, q_recv, back_send, back_recv, lse_send, lse_recv,
):
    ctx = lax.axis_index("ctx")
    ep = lax.axis_index("ep")
    tp = lax.axis_index("tp")
    n = n_ctx * n_ep
    me = ep * n_ctx + ctx
    rows = q_ref.shape[1]
    features = q_ref.shape[2]
    kv_heads = k_ref.shape[2] // HEAD_WIDTH
    group = features // HEAD_WIDTH // kv_heads
    half = rows // 2
    fan = n_ctx // 2
    hidden_width = wg.shape[1]
    chunk_count, _, double_width = part.shape
    chunk_width = double_width // 2
    slots = returned.shape[0]
    places = features // HEAD_WIDTH

    w_copies = [
        pltpu.make_async_copy(src.at[0], dst, w_sem.at[index])
        for index, (src, dst) in enumerate(((wg_hbm, wg), (wu_hbm, wu), (wd_hbm, wd)))
    ]
    for copy in w_copies:
        copy.start()

    barrier = pltpu.get_barrier_semaphore()

    def greet(other):
        @pl.when(other != me)
        def _():
            pl.semaphore_signal(
                barrier, inc=1,
                device_id={"ep": other // n_ctx, "ctx": other % n_ctx},
                device_id_type=MESH,
            )

    each(n, greet)
    for step in range(1, n_tp):
        pl.semaphore_signal(
            barrier, inc=1, device_id={"tp": (tp + step) % n_tp}, device_id_type=MESH
        )
    ids = ids_ref[...]
    slot_row = lax.broadcasted_iota(jnp.int32, (slots, rows), 0)
    choose = jnp.where(ids == slot_row, 1.0, 0.0)
    below = lax.broadcasted_iota(jnp.int32, (rows, rows), 0)
    across = lax.broadcasted_iota(jnp.int32, (rows, rows), 1)
    strict = jnp.where(below < across, 1.0, 0.0).astype(jnp.bfloat16)
    earlier = jnp.dot(choose.astype(jnp.bfloat16), strict, preferred_element_type=jnp.float32)
    slot_index = jnp.sum(earlier * choose, axis=0, keepdims=True).astype(jnp.int32)
    target_row = jnp.where(ids < n_ep, ids * CAP + slot_index, -1)
    spread = jnp.where(target_row == slot_row, 1.0, 0.0).astype(jnp.bfloat16)
    live = n_ep * CAP
    lane_row = lax.broadcasted_iota(jnp.int32, (slots, rows), 1)
    row_place = jnp.sum(
        jnp.where(target_row == slot_row, lane_row, 0), axis=1, keepdims=True
    )
    q_all[...] = jnp.zeros_like(q_all)
    own_span = pl.ds(pl.multiple_of(ctx * slots, 8), slots)
    for start, size in tiles_of(features, 512):
        picked = jnp.dot(
            spread, q_ref[0, :, start:start + size], preferred_element_type=jnp.float32
        )
        q_all[own_span, start:start + size] = picked
        q_out[:, start:start + size] = picked[:live].astype(jnp.bfloat16)

    pl.semaphore_wait(barrier, n - 1 + n_tp - 1)

    def own_copy(piece):
        origin, buf = (k_ref, kbuf) if piece < 2 else (v_ref, vbuf)
        span = pl.ds((piece % 2) * half, half)
        return pltpu.make_async_remote_copy(
            src_ref=origin.at[0, span],
            dst_ref=buf.at[ctx, span],
            send_sem=kv_send.at[ctx, piece],
            recv_sem=kv_recv.at[ctx, piece],
            device_id={"ctx": ctx + 1},
            device_id_type=MESH,
        )

    def block_piece(block, piece):
        buf = kbuf if piece < 2 else vbuf
        span = pl.ds((piece % 2) * half, half)
        return pltpu.make_async_remote_copy(
            src_ref=buf.at[block, span],
            dst_ref=buf.at[block, span],
            send_sem=kv_send.at[block, piece],
            recv_sem=kv_recv.at[block, piece],
            device_id={"ctx": ctx + 1},
            device_id_type=MESH,
        )

    def push_own(first, last):
        @pl.when(ctx < n_ctx - 1)
        def _():
            for piece in range(first, last):
                own_copy(piece).start()

    def relay(block, first, last):
        @pl.when(block >= 0)
        def _():
            for piece in range(first, last):
                copy = block_piece(block, piece)
                copy.wait_recv()

                @pl.when(ctx < n_ctx - 1)
                def _():
                    copy.start()

    def q_copy(source, target):
        return pltpu.make_async_remote_copy(
            src_ref=q_out, dst_ref=q_in.at[source],
            send_sem=q_send.at[target], recv_sem=q_recv.at[source],
            device_id={"ctx": target}, device_id_type=MESH,
        )

    def back_copies(source, target):
        return [
            pltpu.make_async_remote_copy(
                src_ref=out.at[target], dst_ref=into.at[source],
                send_sem=sent.at[target], recv_sem=got.at[source],
                device_id={"ctx": target}, device_id_type=MESH,
            )
            for out, into, sent, got in (
                (part_out, part_got, back_send, back_recv),
                (lse_out, lse_in, lse_send, lse_recv),
            )
        ]

    def lower(body):
        def one(other):
            @pl.when(other < ctx)
            def _():
                body(other)

        each(n_ctx, one)

    def upper(body):
        def one(other):
            @pl.when(other > ctx)
            def _():
                body(other)

        each(n_ctx, one)

    lower(lambda other: q_copy(ctx, other).start())
    push_own(0, 2)

    kbuf[ctx] = k_ref[0]
    vbuf[ctx] = v_ref[0]
    acc[...] = jnp.zeros_like(acc)
    totals[...] = jnp.zeros_like(totals)
    row_max[...] = jnp.full_like(row_max, MASKED)

    query_offset = lax.broadcasted_iota(jnp.int32, (rows, rows), 0)
    key_offset = lax.broadcasted_iota(jnp.int32, (rows, rows), 1)
    offset_gap = query_offset - key_offset

    def process(block):
        visible = offset_gap >= (block - ctx) * rows
        visible = jnp.concatenate([visible] * group, axis=0)
        for head in range(kv_heads):
            lanes = slice(head * HEAD_WIDTH, (head + 1) * HEAD_WIDTH)
            stacked = jnp.concatenate(
                [
                    q_ref[0, :, (head * group + j) * HEAD_WIDTH:(head * group + j + 1) * HEAD_WIDTH]
                    for j in range(group)
                ],
                axis=0,
            )
            raw = lax.dot_general(
                stacked, kbuf[block, :, lanes], (((1,), (1,)), ((), ())),
                preferred_element_type=jnp.float32,
            )
            raw = jnp.where(visible, raw, MASKED)
            old_max = row_max[head]
            new_max = jnp.maximum(old_max, jnp.max(raw, axis=1, keepdims=True))
            factor = jnp.exp2((old_max - new_max) * EXP2_SCALE)
            weights = jnp.exp2((raw - new_max[:, :rows]) * EXP2_SCALE)
            row_max[head] = new_max
            totals[head] = totals[head] * factor + jnp.sum(weights, axis=1, keepdims=True)
            update = jnp.dot(
                weights.astype(jnp.bfloat16), vbuf[block, :, lanes],
                preferred_element_type=jnp.float32,
            )
            acc[head] = acc[head] * factor + update

    part_all[...] = jnp.zeros_like(part_all)
    lse_all[...] = jnp.full_like(lse_all, MASKED)
    source_row = lax.broadcasted_iota(jnp.int32, (n_ctx * slots, 1), 0) // slots
    limit = jnp.where(
        source_row == ctx, jnp.concatenate([row_place] * n_ctx, axis=0), rows
    )
    limit = jnp.concatenate([limit] * group, axis=0)
    upper(lambda other: q_copy(other, other).wait_recv())

    for other in range(n_ctx):
        @pl.when(other > ctx)
        def _():
            q_all[other * slots:other * slots + live, :] = q_in[other].astype(jnp.float32)

    tall = n_ctx * slots
    key_lane = lax.broadcasted_iota(jnp.int32, (group * tall, rows), 1)
    seen = key_lane <= limit
    head_lane = lax.broadcasted_iota(jnp.int32, (tall, 128), 1)
    lse = jnp.zeros((tall, 128), jnp.float32)
    for head in range(kv_heads):
        lanes = slice(head * HEAD_WIDTH, (head + 1) * HEAD_WIDTH)
        stacked = jnp.concatenate(
            [
                q_all[:, (head * group + j) * HEAD_WIDTH:(head * group + j + 1) * HEAD_WIDTH]
                for j in range(group)
            ],
            axis=0,
        ).astype(jnp.bfloat16)
        raw = lax.dot_general(
            stacked, k_ref[0, :, lanes], (((1,), (1,)), ((), ())),
            preferred_element_type=jnp.float32,
        )
        raw = jnp.where(seen, raw, MASKED)
        top = jnp.max(raw, axis=1, keepdims=True)
        weights = jnp.exp2((raw - top) * EXP2_SCALE)
        total = jnp.sum(weights, axis=1, keepdims=True)
        mixed = jnp.dot(
            weights.astype(jnp.bfloat16), v_ref[0, :, lanes],
            preferred_element_type=jnp.float32,
        ) / total
        column = top * EXP2_SCALE + jnp.log2(total)
        for j in range(group):
            place = head * group + j
            lse = jnp.where(head_lane == place, column[j * tall:(j + 1) * tall], lse)
            for other in range(n_ctx):
                first = j * tall + other * slots
                part_out[other, :, place * HEAD_WIDTH:(place + 1) * HEAD_WIDTH] = mixed[
                    first:first + live
                ].astype(jnp.bfloat16)
    for other in range(n_ctx):
        lse_out[other] = lse[other * slots:(other + 1) * slots]

    def give_back(other):
        for copy in back_copies(ctx, other):
            copy.start()

    upper(give_back)
    push_own(2, 4)

    def take_back(other):
        for copy in back_copies(other, other):
            copy.wait_recv()

    lower(take_back)
    for other in range(n_ctx):
        @pl.when(other < ctx)
        def _():
            part_all[other, :live] = part_got[other].astype(jnp.float32)
            lse_all[other] = lse_in[other]

        @pl.when(other == ctx)
        def _():
            part_all[other, :live] = part_out[other].astype(jnp.float32)
            lse_all[other] = lse_out[other]

    peak = jnp.max(lse_all[...], axis=0)
    shares = [jnp.exp2(lse_all[other] - peak) for other in range(n_ctx)]
    share_total = functools.reduce(jnp.add, shares)
    shares = [share / share_total for share in shares]
    for place in range(kv_heads * group):
        span = slice(place * HEAD_WIDTH, (place + 1) * HEAD_WIDTH)
        picked = shares[0][:, place:place + 1] * part_all[0, :, span]
        for other in range(1, n_ctx):
            picked = picked + shares[other][:, place:place + 1] * part_all[other, :, span]
        for expert in range(n_ep):
            out_rows[expert, place * CAP:(place + 1) * CAP] = picked[expert * CAP:(expert + 1) * CAP].astype(
                jnp.bfloat16
            )

    def row_copy(other, source):
        return pltpu.make_async_remote_copy(
            src_ref=out_rows.at[other // n_ctx],
            dst_ref=in_rows.at[source],
            send_sem=row_send.at[other],
            recv_sem=row_recv.at[source],
            device_id={"ep": other // n_ctx, "ctx": other % n_ctx},
            device_id_type=MESH,
        )

    def others(body):
        def one(step):
            @pl.when(step != me)
            def _():
                body(step)

        each(n, one)

    others(lambda other: row_copy(other, me).start())
    in_rows[me] = out_rows[ep]
    process(ctx)
    relay(ctx - 1, 0, 4)
    for copy in w_copies:
        copy.wait()
    others(lambda other: row_copy(other, other).wait_recv())

    def gather_member(index):
        dense = in_rows[index].astype(jnp.float32)
        for place in range(places):
            span = slice(place * HEAD_WIDTH, (place + 1) * HEAD_WIDTH)
            members_f32[index * CAP:(index + 1) * CAP, span] = dense[
                place * CAP:(place + 1) * CAP
            ]

    for index in range(n):
        gather_member(index)
    wide = members_f32[...]
    members = wide.astype(jnp.bfloat16)
    own_score = jnp.sum(wide * router_ref[...].astype(jnp.float32), axis=1, keepdims=True)
    score[...] = jnp.broadcast_to(own_score, score.shape).astype(jnp.bfloat16)
    peer = {"tp": n_tp - 1 - tp}
    score_copy = pltpu.make_async_remote_copy(
        src_ref=score, dst_ref=score_in, send_sem=score_sem.at[0], recv_sem=score_sem.at[1],
        device_id=peer, device_id_type=MESH,
    )
    score_copy.start()
    part_copies = []
    for chunk in range(chunk_count):
        span = slice(chunk * chunk_width, (chunk + 1) * chunk_width)
        part[chunk, :, :chunk_width] = jnp.dot(
            members, wg[:, span], preferred_element_type=jnp.float32
        ).astype(jnp.bfloat16)
        part[chunk, :, chunk_width:] = jnp.dot(
            members, wu[:, span], preferred_element_type=jnp.float32
        ).astype(jnp.bfloat16)
        copy = pltpu.make_async_remote_copy(
            src_ref=part.at[chunk], dst_ref=part_in.at[chunk],
            send_sem=part_send.at[chunk], recv_sem=part_recv.at[chunk],
            device_id=peer, device_id_type=MESH,
        )
        copy.start()
        part_copies.append(copy)
    relay(ctx - 2, 0, 2)
    score_copy.wait()
    gain = jax.nn.sigmoid(
        score[:, :1].astype(jnp.float32) + score_in[:, :1].astype(jnp.float32)
    )
    for chunk, copy in enumerate(part_copies):
        copy.wait()
        both = part[chunk].astype(jnp.float32) + part_in[chunk].astype(jnp.float32)
        gate = gain * both[:, :chunk_width]
        up = gain * both[:, chunk_width:]
        hidden[:, chunk * chunk_width:(chunk + 1) * chunk_width] = (
            gate * jax.nn.sigmoid(gate) * up
        ).astype(jnp.bfloat16)
    for start, size in tiles_of(features, 512):
        product = jnp.dot(
            hidden[...], wd[:, start:start + size], preferred_element_type=jnp.float32
        )
        for index in range(n):
            for place in range(start // HEAD_WIDTH, (start + size) // HEAD_WIDTH):
                lane = place * HEAD_WIDTH - start
                down_out[index, place * CAP:(place + 1) * CAP] = product[
                    index * CAP:(index + 1) * CAP, lane:lane + HEAD_WIDTH
                ].astype(jnp.bfloat16)

    def down_copy(other, source):
        return pltpu.make_async_remote_copy(
            src_ref=down_out.at[other],
            dst_ref=down_in.at[source],
            send_sem=down_send.at[other],
            recv_sem=down_recv.at[source],
            device_id={"ep": other // n_ctx, "ctx": other % n_ctx},
            device_id_type=MESH,
        )

    others(lambda other: down_copy(other, me).start())
    down_in[me] = down_out[me]
    returned[...] = jnp.zeros_like(returned)

    def visit(step, carry):
        block = ctx - step

        @pl.when(step == 2)
        def _():
            relay(block, 2, 4)

        @pl.when(step > 2)
        def _():
            relay(block, 0, 4)

        @pl.when(block >= 0)
        def _():
            process(block)

        return carry

    lax.fori_loop(1, n_ctx, visit, 0)

    for head in range(kv_heads):
        normed = (acc[head] / totals[head]).astype(jnp.bfloat16)
        for j in range(group):
            place = (head * group + j) * HEAD_WIDTH
            att[:, place:place + HEAD_WIDTH] = normed[j * rows:(j + 1) * rows]

    others(lambda other: row_copy(other, me).wait_send())
    lower(lambda other: q_copy(ctx, other).wait_send())

    def sent_back(other):
        for copy in back_copies(ctx, other):
            copy.wait_send()

    upper(sent_back)

    def drain(step, carry):
        block = ctx - step

        @pl.when((ctx < n_ctx - 1) & (block >= 0))
        def _():
            for piece in range(4):
                block_piece(block, piece).wait_send()

        return carry

    lax.fori_loop(0, n_ctx, drain, 0)

    others(lambda other: down_copy(other, other).wait_recv())
    for expert in range(n_ep):
        total = down_in[expert * n_ctx].astype(jnp.float32)
        for index in range(1, n_ctx):
            total = total + down_in[expert * n_ctx + index].astype(jnp.float32)
        total = total.astype(jnp.bfloat16).astype(jnp.float32)
        for place in range(places):
            span = slice(place * HEAD_WIDTH, (place + 1) * HEAD_WIDTH)
            returned[expert * CAP:(expert + 1) * CAP, span] = total[
                place * CAP:(place + 1) * CAP
            ]
    for start, size in tiles_of(features, 512):
        routed = lax.dot_general(
            spread, returned[:, start:start + size].astype(jnp.bfloat16),
            (((0,), (0,)), ((), ())), preferred_element_type=jnp.float32,
        )
        out_ref[0, :, start:start + size] = (
            att[:, start:start + size].astype(jnp.float32) + routed
        ).astype(jnp.bfloat16)
    others(lambda other: down_copy(other, me).wait_send())


def shards(queries, keys, values, expert_ids, router, w_gate, w_up, w_down):
    n_ctx, n_ep, n_tp = (lax.axis_size(axis) for axis in ("ctx", "ep", "tp"))
    n = n_ctx * n_ep
    _, rows, features = queries.shape
    kv_width = keys.shape[2]
    kv_heads = kv_width // HEAD_WIDTH
    group = features // kv_width
    hidden_width = w_gate.shape[2]
    chunk_width = min(hidden_width, 256)
    chunk_count = hidden_width // chunk_width
    members = n * CAP
    dense = features // HEAD_WIDTH * CAP
    live = n_ep * CAP
    slots = -(-live // 8) * 8
    bf16, f32 = jnp.bfloat16, jnp.float32
    vmem = pl.BlockSpec(memory_space=pltpu.VMEM)
    hbm = pl.BlockSpec(memory_space=pl.ANY)
    dma = pltpu.SemaphoreType.DMA
    return pl.pallas_call(
        functools.partial(kernel, n_ctx, n_ep, n_tp),
        out_shape=jax.ShapeDtypeStruct(queries.shape, bf16),
        in_specs=[vmem] * 5 + [hbm] * 3,
        out_specs=vmem,
        scratch_shapes=[
            pltpu.VMEM(w_gate.shape[1:], bf16),
            pltpu.VMEM(w_up.shape[1:], bf16),
            pltpu.VMEM(w_down.shape[1:], bf16),
            pltpu.VMEM((n_ctx, rows, kv_width), bf16),
            pltpu.VMEM((n_ctx, rows, kv_width), bf16),
            pltpu.VMEM((kv_heads, group * rows, HEAD_WIDTH), f32),
            pltpu.VMEM((kv_heads, group * rows, HEAD_WIDTH), f32),
            pltpu.VMEM((kv_heads, group * rows, HEAD_WIDTH), f32),
            pltpu.VMEM((rows, features), bf16),
            pltpu.VMEM((live, features), bf16),
            pltpu.VMEM((n_ctx, live, features), bf16),
            pltpu.VMEM((n_ctx * slots, features), f32),
            pltpu.VMEM((n_ctx, live, features), bf16),
            pltpu.VMEM((n_ctx, live, features), bf16),
            pltpu.VMEM((n_ctx, slots, features), f32),
            pltpu.VMEM((n_ctx, slots, 128), f32),
            pltpu.VMEM((n_ctx, slots, 128), f32),
            pltpu.VMEM((n_ctx, slots, 128), f32),
            pltpu.VMEM((n_ep, dense, HEAD_WIDTH), bf16),
            pltpu.VMEM((n, dense, HEAD_WIDTH), bf16),
            pltpu.VMEM((members, features), f32),
            pltpu.VMEM((chunk_count, members, 2 * chunk_width), bf16),
            pltpu.VMEM((chunk_count, members, 2 * chunk_width), bf16),
            pltpu.VMEM((members, 128), bf16),
            pltpu.VMEM((members, 128), bf16),
            pltpu.VMEM((members, hidden_width), bf16),
            pltpu.VMEM((n, dense, HEAD_WIDTH), bf16),
            pltpu.VMEM((n, dense, HEAD_WIDTH), bf16),
            pltpu.VMEM((slots, features), f32),
            dma((3,)),
            dma((n_ctx, 4)),
            dma((n_ctx, 4)),
            dma((n,)),
            dma((n,)),
            dma((chunk_count,)),
            dma((chunk_count,)),
            dma((2,)),
            dma((n,)),
            dma((n,)),
            dma((n_ctx,)),
            dma((n_ctx,)),
            dma((n_ctx,)),
            dma((n_ctx,)),
            dma((n_ctx,)),
            dma((n_ctx,)),
        ],
        compiler_params=pltpu.CompilerParams(
            collective_id=0, has_side_effects=True, vmem_limit_bytes=60 * 1024 * 1024
        ),
    )(
        expert_ids.reshape(1, rows), router.reshape(1, features), queries, keys, values,
        w_gate, w_up, w_down,
    )


def solution(mesh):
    placed = (
        P(("groups", "ep"), "ctx", "tp"),
        P(("groups", "ep"), "ctx", "tp"),
        P(("groups", "ep"), "ctx", "tp"),
        P(("groups", "ep"), "ctx", None),
        P("tp", "ep"),
        P("ep", "tp", "ctx"),
        P("ep", "tp", "ctx"),
        P("ep", "ctx", "tp"),
    )
    return jax.shard_map(
        shards,
        mesh=mesh,
        in_specs=placed,
        out_specs=P(("groups", "ep"), "ctx", "tp"),
        check_vma=False,
    )
```
